32 devices in a mesh: dom: 4 (over x, core), grp: 8 (over z, y).
Axes of the slice: x: 2, y: 2, z: 4, core: 2. Of those that a mesh axis runs over, the one named last changes fastest.
Arguments:
- features: bfloat16 [131072, 256], P(('dom', 'grp')), may hold values from -6 to 6
- w_fine: bfloat16 [256, 256], replicated, may hold values from -0.375 to 0.375
- adj_tiles: bfloat16 [1024, 20, 128, 128], P(('dom', 'grp')), may hold values from -0.125 to 0.125
- tile_cols: int32 [1024, 20], P(('dom', 'grp')), may hold values from 0 to 39
- tile_count: int32 [1024], P(('dom', 'grp')), may hold values from 1 to 20, as said below
- send_lower: int32 [128], P(('dom', 'grp')), may hold values from 0 to 31
- send_upper: int32 [128], P(('dom', 'grp')), may hold values from 0 to 31
- assign: int32 [131072], P(('dom', 'grp')), may hold values from 0 to 1023, as said below
- w_coarse: bfloat16 [256, 256], replicated, may hold values from -0.375 to 0.375
- coarse_adj: bfloat16 [1024, 1024], P(('dom', 'grp')), may hold values from -0.1875 to 0.1875
Outputs:
- output: bfloat16 [131072, 256], P(('dom', 'grp'))
The draws below stay inside these ranges and needn't reach their ends.
Inputs may be any that keep to these rules, and one draw needn't show every extreme that they name: The first tile_count[r] slots of block row r are live; the others are ignored. `assign`: every coarse node is the coarse node of at least one vertex.
All inputs are finite; a program needn't handle non-finite values.
Results may differ from the reference program's by a relative error of at most 0.011.
Values may be sent and summed in bfloat16 or wider, within the bound.
No kernel may reach another device: no remote copies, remote signals or barrier semaphores. Data moves between devices by JAX's collectives and lax.ppermute only.
A program may use at most 192 MiB of HBM per device.

```python
import jax
import jax.numpy as jnp
from jax import lax

F = 256
BS = 128
K = 20
H = 4
NC = 1024
V_DEV = 4096
NB = 32
NBLK = 1024
VERT = 131072
N_DOM = 4
N_GRP = 8
DEVICES = 32


def draw_tile_count(key, part):
    device_count = NBLK // NB
    key_caps, key_draw, key_star = jax.random.split(key, 3)
    device_caps = jax.random.randint(key_caps, (device_count,), 1, K + 1)
    busiest = jax.random.randint(key_star, (), 0, device_count)
    device_caps = device_caps.at[busiest].set(K)
    raw_draw = jax.random.randint(key_draw, (device_count, NB), 0, K)
    counts = 1 + raw_draw % device_caps[:, None]
    counts = counts.at[busiest, 0].set(K)
    return counts.reshape(NBLK).astype(jnp.int32)


def draw_assign(key, part):
    device_count = VERT // V_DEV
    per_device = NC // device_count
    key_spread = jax.random.fold_in(key, 7)
    position = jnp.arange(VERT, dtype=jnp.int32)
    owner_part = position // V_DEV
    within = position % V_DEV
    spread_node = jax.random.randint(key_spread, (VERT,), 0, NC)
    chosen = jnp.where(within < per_device, owner_part * per_device + within, spread_node)
    return chosen.astype(jnp.int32)


def set_ends(entries, rng, smallest, largest):
    longest = entries.shape.index(max(entries.shape))
    spots = []
    for shift in (0, 1):
        where = [jax.random.randint(jax.random.fold_in(rng, axis), (), 0, length) for axis, length in enumerate(entries.shape)]
        where[longest] = (where[longest] + shift) % entries.shape[longest]
        spots.append(tuple(where))
    return entries.at[spots[0]].set(smallest).at[spots[1]].set(largest)


def block_levels(own_key, dims, shards, low, largest):
    factor_of = 1.0
    for dim, shards_of in shards:
        draws = jax.random.uniform(jax.random.fold_in(jax.random.fold_in(own_key, 6), dim), (shards_of,), jnp.float32, low / len(shards), largest / len(shards))
        factor_of = factor_of * jnp.repeat(jnp.exp(draws), dims[dim] // shards_of).reshape((-1,) + (1,) * (len(dims) - 1 - dim))
    return factor_of


def scatter_about(key, shape, deviation, most, pieces=(), kind=jnp.bfloat16):
    level = block_levels(key, shape, pieces, -0.22, 0.18) if pieces else 1.0
    values = jax.random.normal(key, shape, jnp.float32) * deviation * level
    return jnp.minimum(jnp.maximum(values, -most), most).astype(kind)


def setup_inputs(seed: int = 0) -> dict:
    seeds = jax.random.split(jax.random.key(seed), 11)
    return {
        "features": scatter_about(seeds[0], (VERT, F), 1.0, 6.0, ((0, 32),)),
        "w_fine": scatter_about(seeds[1], (F, F), F ** -0.5, 0.375),
        "adj_tiles": scatter_about(seeds[2], (NBLK, K, BS, BS), (K * BS) ** -0.5, 0.125, ((0, 32),)),
        "tile_cols": set_ends(jax.random.randint(seeds[3], (NBLK, K), 0, NB + 2 * H), jax.random.fold_in(seeds[3], 1), 0, (NB + 2 * H) - 1).astype(jnp.int32),
        "tile_count": draw_tile_count(jax.random.fold_in(seeds[10], 71), 0),
        "send_lower": set_ends(jax.random.randint(seeds[5], (DEVICES * H,), 0, NB), jax.random.fold_in(seeds[5], 1), 0, NB - 1).astype(jnp.int32),
        "send_upper": set_ends(jax.random.randint(seeds[6], (DEVICES * H,), 0, NB), jax.random.fold_in(seeds[6], 1), 0, NB - 1).astype(jnp.int32),
        "assign": draw_assign(jax.random.fold_in(seeds[10], 71), 0),
        "w_coarse": scatter_about(seeds[8], (F, F), F ** -0.5, 0.375),
        "coarse_adj": scatter_about(seeds[9], (NC, NC), NC ** -0.5, 0.1875, ((0, 32),)),
    }


def device_spmm(operands):
    extended, weights, columns, live_count = operands
    live_mask = jnp.arange(K)[None, :] < live_count[:, None]
    kept = jnp.where(live_mask[:, :, None, None], weights.astype(jnp.float32), 0.0)
    picked = extended[columns].astype(jnp.float32)
    return jnp.einsum('rkij,rkjf->rif', kept, picked)

def reference(features, w_fine, adj_tiles, tile_cols, tile_count, send_lower, send_upper, assign, w_coarse, coarse_adj):
    block_count = V_DEV // BS
    device_count = N_DOM * N_GRP
    projected = jnp.dot(features, w_fine, preferred_element_type=jnp.float32).astype(jnp.bfloat16)
    flat_blocks = projected.reshape(device_count * block_count, BS, F)
    offsets = (jnp.arange(device_count, dtype=jnp.int32) * block_count)[:, None]
    lower_sel = flat_blocks[send_lower.reshape(device_count, H) + offsets]
    upper_sel = flat_blocks[send_upper.reshape(device_count, H) + offsets]
    lower_sel = lower_sel.reshape(N_DOM, N_GRP, H, BS, F)
    upper_sel = upper_sel.reshape(N_DOM, N_GRP, H, BS, F)
    from_below = jnp.roll(upper_sel, 1, axis=0)
    from_above = jnp.roll(lower_sel, -1, axis=0)
    own_blocks = projected.reshape(N_DOM, N_GRP, block_count, BS, F)
    extended = jnp.concatenate([own_blocks, from_below, from_above], axis=2)
    extended = extended.reshape(device_count, block_count + 2 * H, BS, F)
    fine_out = lax.map(device_spmm, (extended, adj_tiles.reshape(device_count, block_count, K, BS, BS), tile_cols.reshape(device_count, block_count, K), tile_count.reshape(device_count, block_count)))
    fine_out = fine_out.reshape(V_DEV * device_count, F)
    coarse_sums = jax.ops.segment_sum(features.astype(jnp.float32), assign, num_segments=NC)
    counts = jax.ops.segment_sum(jnp.ones((assign.shape[0],), jnp.float32), assign, num_segments=NC)
    coarse = (coarse_sums / jnp.sqrt(counts)[:, None]).astype(jnp.bfloat16)
    coarse_proj = jnp.dot(coarse, w_coarse, preferred_element_type=jnp.float32).astype(jnp.bfloat16)
    coarse_mixed = (coarse_proj.astype(jnp.float32) + jnp.dot(coarse_adj, coarse_proj, preferred_element_type=jnp.float32)).astype(jnp.bfloat16)
    return jax.nn.relu(fine_out + coarse_mixed[assign].astype(jnp.float32)).astype(jnp.bfloat16)
```

```python
import functools

import jax
import jax.numpy as jnp
from jax import lax
from jax.experimental import pallas as pl
from jax.experimental.pallas import tpu as pltpu
from jax.sharding import PartitionSpec as P

AXES = ("dom", "grp")
F32, BF16, I32 = jnp.float32, jnp.bfloat16, jnp.int32
LANES = 128
EXTRA = 16
PACK = 16
I16 = jnp.int16


def bits_of(count):
    assert count & (count - 1) == 0
    return [1 << i for i in range(count.bit_length() - 1)]


def dot(a, b):
    return jnp.dot(a, b, preferred_element_type=F32)


def cost(flops, nbytes):
    return pl.CostEstimate(flops=int(flops), bytes_accessed=int(nbytes), transcendentals=0)


VMEM = pl.BlockSpec(memory_space=pltpu.VMEM)
SMEM = pl.BlockSpec(memory_space=pltpu.SMEM)
ANY = pl.BlockSpec(memory_space=pltpu.HBM)


def one_hot(packed, rows, first):
    width = packed.shape[1]
    sub = lax.broadcasted_iota(I32, (PACK, width), 0)
    out = []
    for at in range(0, rows, PACK):
        hot = packed == (sub + (first + at)).astype(I16)
        out.append(jnp.where(hot, jnp.ones((), BF16), jnp.zeros((), BF16)))
    return jnp.concatenate(out, axis=0)


def after(x, *others):
    return lax.optimization_barrier((x, *others))[0]


def in_hbm(x):
    return pltpu.with_memory_space_constraint(x, pltpu.HBM)


def sums_kernel(assign_ref, x_hbm, keep_ref, send_ref, x_ref, acc, cnt, tail, sems, *, slots, rows, base, digits, width):
    dom = lax.axis_index("dom")
    chunks = x_ref.shape[0] // width

    def fetch(i):
        at = pl.ds(i * width, width)
        return pltpu.make_async_copy(x_hbm.at[at, :], x_ref.at[at, :], sems.at[i])

    for i in range(chunks):
        fetch(i).start()
    for i in range(chunks):
        nodes = assign_ref[:, i * width : (i + 1) * width]
        packed = jnp.broadcast_to(nodes, (PACK, width)).astype(I16)
        high = lax.broadcasted_iota(I32, (cnt.shape[0], width), 0) == lax.shift_right_logical(nodes, 7)
        low = lax.broadcasted_iota(I32, (LANES, width), 0) == (nodes & (LANES - 1))
        count = lax.dot_general(
            jnp.where(high, 1.0, 0.0).astype(BF16),
            jnp.where(low, 1.0, 0.0).astype(BF16),
            (((1,), (1,)), ((), ())),
            preferred_element_type=F32,
        )
        cnt[...] = count if i == 0 else cnt[...] + count
        fetch(i).wait()
        x = x_ref[i * width : (i + 1) * width, :]
        for p, s in enumerate(slots):
            part = dot(one_hot(packed, rows, (dom ^ s) * rows), x)
            acc[p] = part if i == 0 else acc[p] + part
    per = rows // LANES
    half = len(slots) // 2
    for p, s in enumerate(slots):
        tail[...] = jnp.zeros_like(tail)
        for h in range(per):
            c = cnt[pl.ds((dom ^ s) * per + h, 1), :]
            over = [c] + [jnp.floor((c + 0.5) * (1.0 / base**d)) for d in range(1, digits)]
            for d in range(digits):
                digit = over[d] if d == digits - 1 else over[d] - base * over[d + 1]
                tail[d * per + h : d * per + h + 1, 0:LANES] = digit
        out = keep_ref if p < half else send_ref
        at = (p % half) * (rows + EXTRA)
        out[at : at + rows, :] = acc[p].astype(out.dtype)
        out[at + rows : at + rows + EXTRA, :] = tail[...].astype(out.dtype)


def segment_sums(features, assign, slots, rows, base, digits):
    verts, feat = features.shape
    width = min(verts, 1024)
    half = len(slots) // 2
    shape = (half * (rows + EXTRA), feat)
    nodes = len(slots) * rows
    return pl.pallas_call(
        functools.partial(sums_kernel, slots=slots, rows=rows, base=base, digits=digits, width=width),
        out_shape=(jax.ShapeDtypeStruct(shape, F32), jax.ShapeDtypeStruct(shape, BF16)),
        in_specs=[VMEM, ANY],
        out_specs=(VMEM, VMEM),
        scratch_shapes=[
            pltpu.VMEM((verts, feat), BF16),
            pltpu.VMEM((len(slots), rows, feat), F32),
            pltpu.VMEM((max(16, nodes // LANES), LANES), F32),
            pltpu.VMEM((EXTRA, feat), F32),
            pltpu.SemaphoreType.DMA((verts // width,)),
        ],
        compiler_params=pltpu.CompilerParams(vmem_limit_bytes=16 << 20),
        cost_estimate=cost(2 * nodes * verts * feat, verts * feat * 2),
        name="sums",
    )(assign.reshape(1, verts), in_hbm(features))


def coarse_kernel(keep_ref, recv_ref, w_ref, out_ref, tail, *, rows, base, digits):
    per = rows // LANES
    feat = keep_ref.shape[1]
    tail[...] = keep_ref[rows:, :] + recv_ref[rows:, :].astype(F32)
    done = []
    for h in range(per):
        c = tail[h : h + 1, 0:LANES]
        for d in range(1, digits):
            c = c + tail[d * per + h : d * per + h + 1, 0:LANES] * float(base**d)
        root = jnp.sqrt(jnp.broadcast_to(c, (LANES, LANES)).T)
        at = slice(h * LANES, (h + 1) * LANES)
        total = keep_ref[at, :] + recv_ref[at, :].astype(F32)
        done.append(
            jnp.concatenate(
                [total[:, j : j + LANES] / root for j in range(0, feat, LANES)], axis=1
            ).astype(BF16)
        )
    out_ref[...] = dot(jnp.concatenate(done, axis=0), w_ref[...]).astype(BF16)


def coarse_part(keep, recv, w, rows, base, digits):
    feat = keep.shape[1]
    return pl.pallas_call(
        functools.partial(coarse_kernel, rows=rows, base=base, digits=digits),
        out_shape=jax.ShapeDtypeStruct((rows, feat), BF16),
        in_specs=[VMEM, VMEM, VMEM],
        out_specs=VMEM,
        scratch_shapes=[pltpu.VMEM((EXTRA, feat), F32)],
        compiler_params=pltpu.CompilerParams(vmem_limit_bytes=8 << 20),
        cost_estimate=cost(2 * rows * feat * feat, rows * feat * 8),
        name="coarse",
    )(keep, recv, w)


def mix_kernel(*refs, slots, rows, own, order):
    pa_ref, pb_ref, *pieces, out_ref, proj, wide, own_rows = refs
    dom = lax.axis_index("dom")
    me = dom * lax.axis_size("grp") + lax.axis_index("grp")
    half = len(slots) // 2
    for p, s in enumerate(slots):
        src = pa_ref if p < half else pb_ref
        value = src[(p % half) * rows : (p % half + 1) * rows, :]
        at = pl.multiple_of((dom ^ s) * rows, rows)
        proj[pl.ds(at, rows), :] = value
        wide[pl.ds(at, rows), :] = value.astype(F32)
    for q, t in enumerate(order):
        at = pl.multiple_of((me ^ t) * own, own)
        own_rows[q * own : (q + 1) * own, :] = wide[pl.ds(at, own), :]
    adj = jnp.concatenate([piece[...].astype(F32) for piece in pieces], axis=0).astype(BF16)
    out_ref[...] = (own_rows[...] + dot(adj, proj[...])).astype(BF16)


def mixed_rows(pa, pb, pieces, slots, rows, own, order):
    nodes, feat = len(slots) * rows, pa.shape[1]
    got = len(order) * own
    return pl.pallas_call(
        functools.partial(mix_kernel, slots=slots, rows=rows, own=own, order=order),
        out_shape=jax.ShapeDtypeStruct((got, feat), BF16),
        in_specs=[VMEM] * (2 + len(pieces)),
        out_specs=VMEM,
        scratch_shapes=[
            pltpu.VMEM((nodes, feat), BF16),
            pltpu.VMEM((nodes, feat), F32),
            pltpu.VMEM((got, feat), F32),
        ],
        compiler_params=pltpu.CompilerParams(vmem_limit_bytes=12 << 20),
        cost_estimate=cost(2 * got * nodes * feat, got * nodes * 2),
        name="mix",
    )(pa, pb, *pieces)


def join_kernel(a_ref, b_ref, out_ref):
    rows = a_ref.shape[0]
    out_ref[0:rows, :] = a_ref[...]
    out_ref[rows:, :] = b_ref[...]


def join(a, b):
    shape = (a.shape[0] + b.shape[0], a.shape[1])
    return pl.pallas_call(
        join_kernel,
        out_shape=jax.ShapeDtypeStruct(shape, a.dtype),
        in_specs=[VMEM, VMEM],
        out_specs=VMEM,
        compiler_params=pltpu.CompilerParams(vmem_limit_bytes=4 << 20),
        cost_estimate=cost(shape[0] * shape[1], shape[0] * shape[1] * 4),
        name="join",
    )(a, b)


def proj_kernel(low_idx, up_idx, x_hbm, w_ref, own_ref, low_ref, up_ref, x_ref, sems, *, width):
    chunks = x_ref.shape[0] // width
    block = low_ref.shape[1]

    def fetch(i):
        at = pl.ds(i * width, width)
        return pltpu.make_async_copy(x_hbm.at[at, :], x_ref.at[at, :], sems.at[i])

    for i in range(chunks):
        fetch(i).start()
    w = w_ref[...]
    for i in range(chunks):
        fetch(i).wait()
        done = dot(x_ref[i * width : (i + 1) * width, :], w).astype(BF16)
        own_ref[i * (width // block) : (i + 1) * (width // block)] = done.reshape(width // block, block, done.shape[1])
    for h in range(low_ref.shape[0]):
        low_ref[h] = own_ref[low_idx[h]]
        up_ref[h] = own_ref[up_idx[h]]


def projection(send_lower, send_upper, features, w, block):
    verts, feat = features.shape
    halo = send_lower.shape[0]
    width = min(verts, 1024)
    sent = jax.ShapeDtypeStruct((halo, block, feat), BF16)
    return pl.pallas_call(
        functools.partial(proj_kernel, width=width),
        out_shape=(jax.ShapeDtypeStruct((verts // block, block, feat), BF16), sent, sent),
        in_specs=[SMEM, SMEM, ANY, VMEM],
        out_specs=(VMEM, VMEM, VMEM),
        scratch_shapes=[pltpu.VMEM((verts, feat), BF16), pltpu.SemaphoreType.DMA((verts // width,))],
        compiler_params=pltpu.CompilerParams(vmem_limit_bytes=14 << 20),
        cost_estimate=cost(2 * verts * feat * feat, 4 * verts * feat),
        name="proj",
    )(send_lower, send_upper, in_hbm(features), w)


GROUP = 4
AHEAD = 8


def fine_kernel(cols_ref, live_ref, own_ref, below_ref, above_ref, adj_hbm, out_ref, ext, tiles, sems):
    rows, block = own_ref.shape[0], own_ref.shape[1]
    halo = below_ref.shape[0]

    def groups(r):
        return lax.div(live_ref[r] + (GROUP - 1), GROUP)

    def fetch(r, i):
        slot = lax.rem(r, AHEAD)
        at = pl.ds(i * GROUP, GROUP)
        return pltpu.make_async_copy(adj_hbm.at[r, at], tiles.at[slot, at], sems.at[slot, i])

    def fetch_row(r):
        @pl.loop(0, groups(r))
        def _(i):
            fetch(r, i).start()

    @pl.loop(0, min(AHEAD, rows))
    def _(r):
        fetch_row(r)

    ext[0:rows] = own_ref[...]
    ext[rows : rows + halo] = below_ref[...]
    ext[rows + halo :] = above_ref[...]

    def body(*accs):
        def push(r, i):
            for q in range(2):
                k = i * GROUP + 2 * q
                rhs = jnp.concatenate([ext[cols_ref[k, r]], ext[cols_ref[k + 1, r]]], axis=0)
                pltpu.matmul_push_rhs(rhs, staging_register=0, mxu_index=q)

        def multiply(r, parity):
            live, count, slot = live_ref[r], groups(r), lax.rem(r, AHEAD)

            def one(i, carry):
                fetch(r, i).wait()
                for q in range(2):
                    lhs = []
                    for j in range(2):
                        k = i * GROUP + 2 * q + j
                        tile = tiles[slot, k]
                        lhs.append(jnp.where(k < live, tile, jnp.zeros_like(tile)))
                    pltpu.matmul_acc_lhs(accs[2 * q + parity], jnp.concatenate(lhs, axis=1), load_staged_rhs=0)
                last = i + 1 >= count
                push(jnp.where(last, jnp.minimum(r + 1, rows - 1), r), jnp.where(last, 0, i + 1))
                return carry

            lax.fori_loop(0, count, one, 0)

        def finish(r, parity):
            at = pl.ds(pl.multiple_of(r * block, block), block)
            out_ref[at, :] = pltpu.matmul_pop(accs[parity]) + pltpu.matmul_pop(accs[2 + parity])

            @pl.when(r + AHEAD < rows)
            def _():
                fetch_row(r + AHEAD)

        push(0, 0)
        multiply(0, 0)

        @pl.loop(0, rows // 2 - 1)
        def _(h):
            r = 2 * h
            multiply(r + 1, 1)
            finish(r, 0)
            multiply(r + 2, 0)
            finish(r + 1, 1)

        multiply(rows - 1, 1)
        finish(rows - 2, 0)
        for q in range(2):
            zero = jnp.zeros((block, 2 * block), BF16)
            pltpu.matmul_acc_lhs(accs[2 * q], zero, load_staged_rhs=0)
        finish(rows - 1, 1)
        for q in range(2):
            ext[0, 0:8, :] = pltpu.matmul_pop(accs[2 * q])[0:8].astype(BF16)

    shape = (block, 2 * block)
    pl.run_scoped(body, *[pltpu.ACC(q)(shape, F32) for q in (0, 0, 1, 1)])


def fine_rows(tile_cols, tile_count, own, below, above, adj_tiles):
    rows, slots, block, _ = adj_tiles.shape
    feat = own.shape[2]
    halo = below.shape[0]
    assert slots % GROUP == 0 and rows % 2 == 0 and feat == 2 * block
    return pl.pallas_call(
        fine_kernel,
        out_shape=jax.ShapeDtypeStruct((rows * block, feat), F32),
        in_specs=[SMEM, SMEM, VMEM, VMEM, VMEM, ANY],
        out_specs=VMEM,
        scratch_shapes=[
            pltpu.VMEM((rows + 2 * halo, block, feat), BF16),
            pltpu.VMEM((AHEAD, slots, block, block), BF16),
            pltpu.SemaphoreType.DMA((AHEAD, slots // GROUP)),
        ],
        compiler_params=pltpu.CompilerParams(vmem_limit_bytes=24 << 20),
        cost_estimate=cost(2 * rows * slots * block * block * feat, rows * slots * block * block * 2),
        name="fine",
    )(tile_cols.T, tile_count, own, below, above, in_hbm(adj_tiles))


def out_kernel(assign_ref, ma_ref, mb_ref, fine_ref, out_hbm, out_ref, sems, *, own, gather_bits, width):
    me = lax.axis_index("dom") * lax.axis_size("grp") + lax.axis_index("grp")
    shift = own.bit_length() - 1
    assign = assign_ref[...]
    apart = lax.shift_right_logical(assign, shift) ^ me
    place = assign & (own - 1)
    for j, bit in enumerate(gather_bits):
        place = place + jnp.where((apart & bit) != 0, own << j, 0)
    place = place.astype(F32)
    nodes = ma_ref.shape[0] + mb_ref.shape[0]
    mixed = jnp.concatenate([ma_ref[...], mb_ref[...]], axis=0)
    lane = lax.broadcasted_iota(I32, (LANES, nodes), 1).astype(I16)
    chunks = out_ref.shape[0] // width

    def store(i):
        at = pl.ds(i * width, width)
        return pltpu.make_async_copy(out_ref.at[at, :], out_hbm.at[at, :], sems.at[i])

    for i in range(chunks):
        hots = []
        for j in range(i * width // LANES, (i + 1) * width // LANES):
            column = jnp.broadcast_to(place[j : j + 1, :], (LANES, LANES)).T.astype(I32).astype(I16)
            hot = jnp.concatenate([column] * (nodes // LANES), axis=1) == lane
            hots.append(jnp.where(hot, jnp.ones((), BF16), jnp.zeros((), BF16)))
        picked = dot(jnp.concatenate(hots, axis=0), mixed)
        at = slice(i * width, (i + 1) * width)
        out_ref[at, :] = jnp.maximum(fine_ref[at, :] + picked, 0.0).astype(BF16)
        store(i).start()
    for i in range(chunks):
        store(i).wait()


def output_rows(assign, ma, mb, fine, own, gather_bits):
    verts, feat = fine.shape
    width = min(verts, 1024)
    nodes = ma.shape[0] + mb.shape[0]
    return pl.pallas_call(
        functools.partial(out_kernel, own=own, gather_bits=gather_bits, width=width),
        out_shape=jax.ShapeDtypeStruct((verts, feat), BF16),
        in_specs=[VMEM, VMEM, VMEM, VMEM],
        out_specs=ANY,
        scratch_shapes=[pltpu.VMEM((verts, feat), BF16), pltpu.SemaphoreType.DMA((verts // width,))],
        compiler_params=pltpu.CompilerParams(vmem_limit_bytes=24 << 20),
        cost_estimate=cost(2 * verts * nodes * feat, verts * feat * 6),
        name="out",
    )(assign.reshape(verts // LANES, LANES), ma, mb, fine)


def per_device(
    features,
    w_fine,
    adj_tiles,
    tile_cols,
    tile_count,
    send_lower,
    send_upper,
    assign,
    w_coarse,
    coarse_adj,
):
    verts, feat = features.shape
    block = adj_tiles.shape[2]
    own, nodes = coarse_adj.shape
    doms, grps = lax.axis_size("dom"), lax.axis_size("grp")
    devices = doms * grps
    dom_bits, grp_bits = bits_of(doms), bits_of(grps)
    rows = nodes // doms

    def flip(x, bit):
        return lax.ppermute(x, AXES, [(i, i ^ bit) for i in range(devices)])

    base = 256 // devices + 1
    digits = 1
    while base**digits <= verts:
        digits += 1

    slots = [0]
    for bit in dom_bits[::-1]:
        slots = slots + [s ^ bit for s in slots]

    gather_bits = grp_bits[:0:-1] + [b * grps for b in dom_bits[:0:-1]] + grp_bits[:1]
    last_bit = dom_bits[0] * grps
    order = [0]
    for bit in gather_bits:
        order = order + [t ^ bit for t in order]
    pieces = [coarse_adj]
    pending = iter(gather_bits)

    def gather_step(block_, *deps):
        bit = next(pending, None)
        if bit is None:
            return block_
        if deps:
            block_ = after(block_, *deps)
        got = flip(block_, bit)
        pieces.append(got)
        return join(block_, got) if len(pieces) <= len(gather_bits) else block_

    keep, send = segment_sums(features, assign, slots, rows, base, digits)
    recv = flip(send, last_bit)
    coming = gather_step(coarse_adj, send)

    window = 0
    for bit in dom_bits[1:]:
        total = keep + recv.astype(F32)
        half = total.shape[0] // 2
        keep, send = total[:half], total[half:].astype(BF16)
        recv = flip(send, bit * grps)
        if window == 0:
            projected, low, up = projection(send_lower, send_upper, after(features, send), w_fine, block)
            coming = gather_step(coming, projected)
            keep = after(keep, projected)
        window += 1
    for step, bit in enumerate(grp_bits):
        keep = keep + recv.astype(F32)
        send = keep.astype(BF16)
        if step == 0:
            low, up = after(low, send), after(up, send)
            going_up = [(i, (i + 1) % doms) for i in range(doms)]
            from_below = lax.ppermute(up, "dom", going_up)
            from_above = lax.ppermute(low, "dom", [(j, i) for i, j in going_up])
        recv = flip(send, bit)
        if step > 0:
            coming = gather_step(coming, send)
        if step == len(grp_bits) - 1:
            fine = fine_rows(tile_cols, tile_count, after(projected, send), from_below, from_above, adj_tiles)
            keep, fine = lax.optimization_barrier((keep, fine))
    while len(pieces) <= len(gather_bits):
        coming = gather_step(coming)
    proj = coarse_part(keep, recv, w_coarse, rows, base, digits)
    for bit in dom_bits[:0:-1]:
        proj = join(proj, flip(proj, bit * grps))
    other = flip(proj, last_bit)
    mixed = mixed_rows(proj, other, pieces, slots, rows, own, order)
    mixed_other = flip(mixed, last_bit)
    return output_rows(assign, mixed, mixed_other, fine, own, gather_bits + [last_bit])


def solution(mesh):
    return jax.shard_map(
        per_device,
        mesh=mesh,
        in_specs=(
            P(AXES, None),
            P(),
            P(AXES, None, None, None),
            P(AXES, None),
            P(AXES),
            P(AXES),
            P(AXES),
            P(AXES),
            P(),
            P(AXES, None),
        ),
        out_specs=P(AXES, None),
        check_vma=False,
    )
```

```python
import functools

import jax
import jax.numpy as jnp
from jax import lax
from jax.experimental import pallas as pl
from jax.experimental.pallas import tpu as pltpu
from jax.sharding import PartitionSpec as P


AXES = ("dom", "grp")
F32, BF16, I32 = jnp.float32, jnp.bfloat16, jnp.int32
LANES = 128
EXTRA = 16
PACK = 16
I16 = jnp.int16


def bits_of(count):
    assert count & (count - 1) == 0
    return [1 << i for i in range(count.bit_length() - 1)]


def dot(a, b):
    return jnp.dot(a, b, preferred_element_type=F32)


def cost(flops, nbytes):
    return pl.CostEstimate(flops=int(flops), bytes_accessed=int(nbytes), transcendentals=0)


VMEM = pl.BlockSpec(memory_space=pltpu.VMEM)
SMEM = pl.BlockSpec(memory_space=pltpu.SMEM)
ANY = pl.BlockSpec(memory_space=pltpu.HBM)


def one_hot(packed, rows, first):
    width = packed.shape[1]
    sub = lax.broadcasted_iota(I32, (PACK, width), 0)
    out = []
    for at in range(0, rows, PACK):
        hot = packed == (sub + (first + at)).astype(I16)
        out.append(jnp.where(hot, jnp.ones((), BF16), jnp.zeros((), BF16)))
    return jnp.concatenate(out, axis=0)


def in_hbm(x):
    return pltpu.with_memory_space_constraint(x, pltpu.HBM)


def sums_kernel(
    assign_hbm, x_hbm, keep_ref, send_ref, x_ref, assign_ref, acc, cnt, tail, sems, *, slots, rows, base, digits, width
):
    dom = lax.axis_index("dom")
    chunks = x_ref.shape[0] // width

    def fetch(i):
        at = pl.ds(i * width, width)
        return pltpu.make_async_copy(x_hbm.at[at, :], x_ref.at[at, :], sems.at[i])

    ids = pltpu.make_async_copy(assign_hbm, assign_ref, sems.at[chunks])
    ids.start()
    for i in range(chunks):
        fetch(i).start()
    ids.wait()
    for i in range(chunks):
        nodes = assign_ref[:, i * width : (i + 1) * width]
        packed = jnp.broadcast_to(nodes, (PACK, width)).astype(I16)
        high = lax.broadcasted_iota(I32, (cnt.shape[0], width), 0) == lax.shift_right_logical(nodes, 7)
        low = lax.broadcasted_iota(I32, (LANES, width), 0) == (nodes & (LANES - 1))
        count = lax.dot_general(
            jnp.where(high, 1.0, 0.0).astype(BF16),
            jnp.where(low, 1.0, 0.0).astype(BF16),
            (((1,), (1,)), ((), ())),
            preferred_element_type=F32,
        )
        cnt[...] = count if i == 0 else cnt[...] + count
        fetch(i).wait()
        x = x_ref[i * width : (i + 1) * width, :]
        for p, s in enumerate(slots):
            part = dot(one_hot(packed, rows, (dom ^ s) * rows), x)
            acc[p] = part if i == 0 else acc[p] + part
    per = rows // LANES
    half = len(slots) // 2
    for p, s in enumerate(slots):
        tail[...] = jnp.zeros_like(tail)
        for h in range(per):
            c = cnt[pl.ds((dom ^ s) * per + h, 1), :]
            over = [c] + [jnp.floor((c + 0.5) * (1.0 / base**d)) for d in range(1, digits)]
            for d in range(digits):
                digit = over[d] if d == digits - 1 else over[d] - base * over[d + 1]
                tail[d * per + h : d * per + h + 1, 0:LANES] = digit
        out = keep_ref if p < half else send_ref
        at = (p % half) * (rows + EXTRA)
        out[at : at + rows, :] = acc[p].astype(out.dtype)
        out[at + rows : at + rows + EXTRA, :] = tail[...].astype(out.dtype)


def segment_sums(features, assign, slots, rows, base, digits):
    verts, feat = features.shape
    width = min(verts, 1024)
    half = len(slots) // 2
    shape = (half * (rows + EXTRA), feat)
    nodes = len(slots) * rows
    return pl.pallas_call(
        functools.partial(sums_kernel, slots=slots, rows=rows, base=base, digits=digits, width=width),
        out_shape=(
            jax.ShapeDtypeStruct(shape, F32),
            jax.ShapeDtypeStruct(shape, BF16),
            jax.ShapeDtypeStruct((verts, feat), BF16),
        ),
        in_specs=[ANY, ANY],
        out_specs=(VMEM, VMEM, VMEM),
        scratch_shapes=[
            pltpu.VMEM((1, verts), I32),
            pltpu.VMEM((len(slots), rows, feat), F32),
            pltpu.VMEM((max(16, nodes // LANES), LANES), F32),
            pltpu.VMEM((EXTRA, feat), F32),
            pltpu.SemaphoreType.DMA((verts // width + 1,)),
        ],
        compiler_params=pltpu.CompilerParams(vmem_limit_bytes=16 << 20),
        cost_estimate=cost(2 * nodes * verts * feat, verts * feat * 2),
        name="sums",
    )(in_hbm(assign.reshape(1, verts)), in_hbm(features))


def coarse_kernel(keep_ref, recv_ref, w_ref, out_ref, tail, *, rows, base, digits):
    per = rows // LANES
    feat = keep_ref.shape[1]
    tail[...] = keep_ref[rows:, :] + recv_ref[rows:, :].astype(F32)
    done = []
    for h in range(per):
        c = tail[h : h + 1, 0:LANES]
        for d in range(1, digits):
            c = c + tail[d * per + h : d * per + h + 1, 0:LANES] * float(base**d)
        root = jnp.sqrt(jnp.broadcast_to(c, (LANES, LANES)).T)
        at = slice(h * LANES, (h + 1) * LANES)
        total = keep_ref[at, :] + recv_ref[at, :].astype(F32)
        done.append(
            jnp.concatenate(
                [total[:, j : j + LANES] / root for j in range(0, feat, LANES)], axis=1
            ).astype(BF16)
        )
    out_ref[...] = dot(jnp.concatenate(done, axis=0), w_ref[...]).astype(BF16)


def coarse_part(keep, recv, w, rows, base, digits):
    feat = keep.shape[1]
    return pl.pallas_call(
        functools.partial(coarse_kernel, rows=rows, base=base, digits=digits),
        out_shape=jax.ShapeDtypeStruct((rows, feat), BF16),
        in_specs=[VMEM, VMEM, VMEM],
        out_specs=VMEM,
        scratch_shapes=[pltpu.VMEM((EXTRA, feat), F32)],
        compiler_params=pltpu.CompilerParams(vmem_limit_bytes=8 << 20),
        cost_estimate=cost(2 * rows * feat * feat, rows * feat * 8),
        name="coarse",
    )(keep, recv, w)


def mix_kernel(*refs, slots, rows, own, order):
    pa_ref, pb_ref, *pieces, out_ref, proj, wide, own_rows = refs
    dom = lax.axis_index("dom")
    me = dom * lax.axis_size("grp") + lax.axis_index("grp")
    half = len(slots) // 2
    for p, s in enumerate(slots):
        src = pa_ref if p < half else pb_ref
        value = src[(p % half) * rows : (p % half + 1) * rows, :]
        at = pl.multiple_of((dom ^ s) * rows, rows)
        proj[pl.ds(at, rows), :] = value
        wide[pl.ds(at, rows), :] = value.astype(F32)
    for q, t in enumerate(order):
        at = pl.multiple_of((me ^ t) * own, own)
        own_rows[q * own : (q + 1) * own, :] = wide[pl.ds(at, own), :]
    adj = jnp.concatenate([piece[...].astype(F32) for piece in pieces], axis=0).astype(BF16)
    out_ref[...] = (own_rows[...] + dot(adj, proj[...])).astype(BF16)


def mixed_rows(pa, pb, pieces, slots, rows, own, order):
    nodes, feat = len(slots) * rows, pa.shape[1]
    got = len(order) * own
    return pl.pallas_call(
        functools.partial(mix_kernel, slots=slots, rows=rows, own=own, order=order),
        out_shape=jax.ShapeDtypeStruct((got, feat), BF16),
        in_specs=[VMEM] * (2 + len(pieces)),
        out_specs=VMEM,
        scratch_shapes=[
            pltpu.VMEM((nodes, feat), BF16),
            pltpu.VMEM((nodes, feat), F32),
            pltpu.VMEM((got, feat), F32),
        ],
        compiler_params=pltpu.CompilerParams(vmem_limit_bytes=12 << 20),
        cost_estimate=cost(2 * got * nodes * feat, got * nodes * 2),
        name="mix",
    )(pa, pb, *pieces)


def join_kernel(a_ref, b_ref, out_ref):
    rows = a_ref.shape[0]
    out_ref[0:rows, :] = a_ref[...]
    out_ref[rows:, :] = b_ref[...]


def join(a, b):
    shape = (a.shape[0] + b.shape[0], a.shape[1])
    return pl.pallas_call(
        join_kernel,
        out_shape=jax.ShapeDtypeStruct(shape, a.dtype),
        in_specs=[VMEM, VMEM],
        out_specs=VMEM,
        compiler_params=pltpu.CompilerParams(vmem_limit_bytes=4 << 20),
        cost_estimate=cost(shape[0] * shape[1], shape[0] * shape[1] * 4),
        name="join",
    )(a, b)


def proj_kernel(low_idx, up_idx, x_ref, w_ref, own_ref, low_ref, up_ref, *, width):
    chunks = x_ref.shape[0] // width
    block = low_ref.shape[1]
    w = w_ref[...]
    for i in range(chunks):
        done = dot(x_ref[i * width : (i + 1) * width, :], w).astype(BF16)
        own_ref[i * (width // block) : (i + 1) * (width // block)] = done.reshape(width // block, block, done.shape[1])
    for h in range(low_ref.shape[0]):
        low_ref[h] = own_ref[low_idx[h]]
        up_ref[h] = own_ref[up_idx[h]]


def projection(send_lower, send_upper, features, w, block):
    verts, feat = features.shape
    halo = send_lower.shape[0]
    sent = jax.ShapeDtypeStruct((halo, block, feat), BF16)
    return pl.pallas_call(
        functools.partial(proj_kernel, width=min(verts, 1024)),
        out_shape=(jax.ShapeDtypeStruct((verts // block, block, feat), BF16), sent, sent),
        in_specs=[SMEM, SMEM, VMEM, VMEM],
        out_specs=(VMEM, VMEM, VMEM),
        compiler_params=pltpu.CompilerParams(vmem_limit_bytes=14 << 20),
        cost_estimate=cost(2 * verts * feat * feat, 4 * verts * feat),
        name="proj",
    )(send_lower, send_upper, features, w)


GROUP = 4
TURNS = 3
LAG = 2


def fine_kernel(cols_ref, live_ref, own_ref, below_ref, above_ref, adj_hbm, out_ref, ext, tiles, sems):
    rows, block = own_ref.shape[0], own_ref.shape[1]
    halo = below_ref.shape[0]

    def groups(r):
        return lax.div(live_ref[r] + (GROUP - 1), GROUP)

    def fetch(r, i):
        at = pl.ds(i * GROUP, GROUP)
        return pltpu.make_async_copy(adj_hbm.at[r, at], tiles.at[r, at], sems.at[r, i])

    @pl.loop(0, rows)
    def _(r):
        @pl.loop(0, groups(r))
        def _(i):
            fetch(r, i).start()

    ext[0:rows] = own_ref[...]
    ext[rows : rows + halo] = below_ref[...]
    ext[rows + halo :] = above_ref[...]

    def body(*accs):
        def push(columns):
            for q in range(2):
                rhs = jnp.concatenate([ext[c] for c in columns[2 * q : 2 * q + 2]], axis=0)
                pltpu.matmul_push_rhs(rhs, staging_register=0, mxu_index=q)

        def columns_of(r, i):
            return [cols_ref[i * GROUP + j, r] for j in range(GROUP)]

        def finish(r, turn):
            at = pl.ds(pl.multiple_of(r * block, block), block)
            out_ref[at, :] = pltpu.matmul_pop(accs[turn]) + pltpu.matmul_pop(accs[TURNS + turn])

        def row(r, turn, before):
            live = live_ref[r]
            following = jnp.minimum(r + 1, rows - 1)

            def with_groups(count):
                def run():
                    for i in range(count):
                        fetch(r, i).wait()
                    for i in range(count):
                        coming = columns_of(following, 0) if i + 1 == count else columns_of(r, i + 1)
                        for q in range(2):
                            lhs = []
                            for j in range(2):
                                k = i * GROUP + 2 * q + j
                                tile = tiles[r, k]
                                if i + 1 == count and 2 * q + j > 0:
                                    tile = jnp.where(k < live, tile, jnp.zeros_like(tile))
                                lhs.append(tile)
                            lhs = jnp.concatenate(lhs, axis=1)
                            pltpu.matmul_acc_lhs(accs[q * TURNS + turn], lhs, load_staged_rhs=0)
                        push(coming)
                        if i == 0 and before is not None:
                            finish(before, (turn + TURNS - LAG) % TURNS)

                return run

            lax.switch(groups(r) - 1, [with_groups(n + 1) for n in range(cols_ref.shape[0] // GROUP)])

        push(columns_of(0, 0))
        for r in range(LAG):
            row(r, r % TURNS, None)

        @pl.loop(0, (rows - LAG) // TURNS)
        def _(h):
            for turn in range(TURNS):
                r = h * TURNS + turn + LAG
                row(r, (turn + LAG) % TURNS, r - LAG)

        for r in range((rows - LAG) // TURNS * TURNS + LAG, rows):
            row(r, r % TURNS, r - LAG)
        spare = rows % TURNS
        for q in range(2):
            zero = jnp.zeros((block, 2 * block), BF16)
            pltpu.matmul_acc_lhs(accs[q * TURNS + spare], zero, load_staged_rhs=0)
        for r in range(rows - LAG, rows):
            finish(r, r % TURNS)
        for q in range(2):
            ext[0, 0:16, :] = pltpu.matmul_pop(accs[q * TURNS + spare])[0:16].astype(BF16)

    shape = (block, 2 * block)
    pl.run_scoped(body, *[pltpu.ACC(q)(shape, F32) for q in range(2) for _ in range(TURNS)])


def fine_rows(tile_cols, tile_count, own, below, above, adj_tiles):
    rows, slots, block, _ = adj_tiles.shape
    feat = own.shape[2]
    halo = below.shape[0]
    assert slots % GROUP == 0 and rows % 2 == 0 and feat == 2 * block
    return pl.pallas_call(
        fine_kernel,
        out_shape=jax.ShapeDtypeStruct((rows * block, feat), F32),
        in_specs=[SMEM, SMEM, VMEM, VMEM, VMEM, ANY],
        out_specs=VMEM,
        scratch_shapes=[
            pltpu.VMEM((rows + 2 * halo, block, feat), BF16),
            pltpu.VMEM((rows, slots, block, block), BF16),
            pltpu.SemaphoreType.DMA((rows, slots // GROUP)),
        ],
        compiler_params=pltpu.CompilerParams(vmem_limit_bytes=36 << 20),
        cost_estimate=cost(2 * rows * slots * block * block * feat, rows * slots * block * block * 2),
        name="fine",
    )(tile_cols.T, tile_count, own, below, above, in_hbm(adj_tiles))


def picked_rows(columns, m_ref, first):
    nodes = m_ref.shape[0]
    lane = (lax.broadcasted_iota(I32, (LANES, nodes), 1) + first).astype(I16)
    hots = []
    for column in columns:
        hot = jnp.concatenate([column] * (nodes // LANES), axis=1) == lane
        hots.append(jnp.where(hot, jnp.ones((), BF16), jnp.zeros((), BF16)))
    return dot(jnp.concatenate(hots, axis=0), m_ref[...])


def place_kernel(assign_ref, m_ref, fine_ref, out_ref, place_ref, *, own, gather_bits, width):
    me = lax.axis_index("dom") * lax.axis_size("grp") + lax.axis_index("grp")
    shift = own.bit_length() - 1
    assign = assign_ref[...]
    apart = lax.shift_right_logical(assign, shift) ^ me
    place = assign & (own - 1)
    for j, bit in enumerate(gather_bits):
        place = place + jnp.where((apart & bit) != 0, own << j, 0)
    place = place.astype(F32)
    for i in range(0, out_ref.shape[0], width):
        columns = []
        for j in range(i // LANES, (i + width) // LANES):
            column = jnp.broadcast_to(place[j : j + 1, :], (LANES, LANES)).T.astype(I32).astype(I16)
            place_ref[j * LANES : (j + 1) * LANES, :] = column
            columns.append(column)
        out_ref[i : i + width, :] = fine_ref[i : i + width, :] + picked_rows(columns, m_ref, 0)


def stored_columns(place_ref, start, width):
    return [place_ref[j : j + LANES, :] for j in range(start, start + width, LANES)]


def gain_kernel(place_ref, m_ref, fine_ref, out_ref, *, first, width):
    for i in range(0, out_ref.shape[0], width):
        columns = stored_columns(place_ref, i, width)
        out_ref[i : i + width, :] = fine_ref[i : i + width, :] + picked_rows(columns, m_ref, first)


def out_kernel(place_ref, m_ref, fine_ref, out_hbm, out_ref, sems, *, first, width):
    chunks = out_ref.shape[0] // width

    def store(i):
        at = pl.ds(i * width, width)
        return pltpu.make_async_copy(out_ref.at[at, :], out_hbm.at[at, :], sems.at[i])

    for i in range(chunks):
        at = slice(i * width, (i + 1) * width)
        picked = picked_rows(stored_columns(place_ref, i * width, width), m_ref, first)
        out_ref[at, :] = jnp.maximum(fine_ref[at, :] + picked, 0.0).astype(BF16)
        store(i).start()
    for i in range(chunks):
        store(i).wait()


def output_rows(assign, part_of, count, fine, own, gather_bits):
    verts, feat = fine.shape
    width = min(verts, 1024)
    place, first = None, 0
    for step in range(count):
        m = part_of(step)
        nodes = m.shape[0]
        shared = dict(
            compiler_params=pltpu.CompilerParams(vmem_limit_bytes=16 << 20),
            cost_estimate=cost(2 * verts * nodes * feat, verts * feat * 6),
        )
        wide = jax.ShapeDtypeStruct((verts, feat), F32)
        if step == 0:
            fine, place = pl.pallas_call(
                functools.partial(place_kernel, own=own, gather_bits=gather_bits, width=width),
                out_shape=(wide, jax.ShapeDtypeStruct((verts, LANES), I16)),
                in_specs=[VMEM] * 3,
                out_specs=(VMEM, VMEM),
                name="place",
                **shared,
            )(assign.reshape(verts // LANES, LANES), m, fine)
        elif step + 1 < count:
            fine = pl.pallas_call(
                functools.partial(gain_kernel, first=first, width=width),
                out_shape=wide,
                in_specs=[VMEM] * 3,
                out_specs=VMEM,
                name="gain",
                **shared,
            )(place, m, fine)
        else:
            return pl.pallas_call(
                functools.partial(out_kernel, first=first, width=width),
                out_shape=jax.ShapeDtypeStruct((verts, feat), BF16),
                in_specs=[VMEM] * 3,
                out_specs=ANY,
                scratch_shapes=[pltpu.VMEM((verts, feat), BF16), pltpu.SemaphoreType.DMA((verts // width,))],
                name="out",
                **shared,
            )(place, m, fine)
        first += nodes


def spread(x, dom_bits, grps, flip):
    parts = [x]
    bits = dom_bits[:0:-1] + dom_bits[:1]
    for step, bit in enumerate(bits):
        parts.append(flip(x, bit * grps))
        if step + 1 < len(bits):
            x = join(x, parts[-1])
    return x, parts


def layer(
    features,
    w_fine,
    adj_tiles,
    tile_cols,
    tile_count,
    send_lower,
    send_upper,
    assign,
    w_coarse,
    coarse_adj,
):
    verts, _ = features.shape
    block = adj_tiles.shape[2]
    own, nodes = coarse_adj.shape
    doms, grps = lax.axis_size("dom"), lax.axis_size("grp")
    devices = doms * grps
    dom_bits, grp_bits = bits_of(doms), bits_of(grps)
    rows = nodes // doms

    def flip(x, bit):
        return lax.ppermute(x, AXES, [(i, i ^ bit) for i in range(devices)])

    base = 256 // devices + 1
    digits = 1
    while base**digits <= verts:
        digits += 1

    slots = [0]
    for bit in dom_bits[::-1]:
        slots = slots + [s ^ bit for s in slots]

    gather_bits = grp_bits[:1:-1] + grp_bits[:1] + grp_bits[1:2]
    order = [0]
    for bit in gather_bits:
        order = order + [t ^ bit for t in order]
    pieces, coming = [coarse_adj], coarse_adj
    for step, bit in enumerate(gather_bits):
        pieces.append(flip(coming, bit))
        if step + 1 < len(gather_bits):
            coming = join(coming, pieces[-1])

    keep, send, held = segment_sums(features, assign, slots, rows, base, digits)
    for step, bit in enumerate(dom_bits):
        recv = flip(send, bit * grps)
        if step + 1 < len(dom_bits):
            total = keep + recv.astype(F32)
            half = total.shape[0] // 2
            keep, send = total[:half], total[half:].astype(BF16)

    projected, low, up = projection(send_lower, send_upper, held, w_fine, block)
    going_up = [(i, (i + 1) % doms) for i in range(doms)]
    from_below = lax.ppermute(up, "dom", going_up)
    from_above = lax.ppermute(low, "dom", [(j, i) for i, j in going_up])
    fine = fine_rows(tile_cols, tile_count, projected, from_below, from_above, adj_tiles)

    for bit in grp_bits:
        keep = keep + recv.astype(F32)
        recv = flip(keep.astype(BF16), bit)
    proj = coarse_part(keep, recv, w_coarse, rows, base, digits)
    proj, parts = spread(proj, dom_bits, grps, flip)
    mixed = mixed_rows(proj, parts[-1], pieces, slots, rows, own, order)
    _, parts = spread(mixed, dom_bits, grps, flip)
    all_bits = gather_bits + [b * grps for b in dom_bits[:0:-1] + dom_bits[:1]]
    return output_rows(assign, lambda i: parts[i], len(parts), fine, own, all_bits)


def solution(mesh):
    return jax.shard_map(
        layer,
        mesh=mesh,
        in_specs=(
            P(AXES, None),
            P(),
            P(AXES, None, None, None),
            P(AXES, None),
            P(AXES),
            P(AXES),
            P(AXES),
            P(AXES),
            P(),
            P(AXES, None),
        ),
        out_specs=P(AXES, None),
        check_vma=False,
    )
```

```python
import functools

import jax
import jax.numpy as jnp
from jax import lax
from jax.experimental import pallas as pl
from jax.experimental.pallas import tpu as pltpu
from jax.sharding import PartitionSpec as P


AXES = ("dom", "grp")
F32, BF16, I32 = jnp.float32, jnp.bfloat16, jnp.int32
LANES = 128
EXTRA = 16
PACK = 16
I16 = jnp.int16


def bits_of(count):
    assert count & (count - 1) == 0
    return [1 << i for i in range(count.bit_length() - 1)]


def dot(a, b):
    return jnp.dot(a, b, preferred_element_type=F32)


def cost(flops, nbytes):
    return pl.CostEstimate(flops=int(flops), bytes_accessed=int(nbytes), transcendentals=0)


VMEM = pl.BlockSpec(memory_space=pltpu.VMEM)
SMEM = pl.BlockSpec(memory_space=pltpu.SMEM)
ANY = pl.BlockSpec(memory_space=pltpu.HBM)


def one_hot(packed, rows, first):
    width = packed.shape[1]
    sub = lax.broadcasted_iota(I32, (PACK, width), 0)
    out = []
    for at in range(0, rows, PACK):
        hot = packed == (sub + (first + at)).astype(I16)
        out.append(jnp.where(hot, jnp.ones((), BF16), jnp.zeros((), BF16)))
    return jnp.concatenate(out, axis=0)


def in_hbm(x):
    return pltpu.with_memory_space_constraint(x, pltpu.HBM)


def sums_kernel(
    assign_hbm, x_hbm, keep_ref, send_ref, x_ref, assign_ref, acc, cnt, tail, sems, *, slots, rows, base, digits, width
):
    dom = lax.axis_index("dom")
    chunks = x_ref.shape[0] // width

    def fetch(i):
        at = pl.ds(i * width, width)
        return pltpu.make_async_copy(x_hbm.at[at, :], x_ref.at[at, :], sems.at[i])

    ids = pltpu.make_async_copy(assign_hbm, assign_ref, sems.at[chunks])
    ids.start()
    for i in range(chunks):
        fetch(i).start()
    ids.wait()
    for i in range(chunks):
        nodes = assign_ref[:, i * width : (i + 1) * width]
        packed = jnp.broadcast_to(nodes, (PACK, width)).astype(I16)
        high = lax.broadcasted_iota(I32, (cnt.shape[0], width), 0) == lax.shift_right_logical(nodes, 7)
        low = lax.broadcasted_iota(I32, (LANES, width), 0) == (nodes & (LANES - 1))
        count = lax.dot_general(
            jnp.where(high, 1.0, 0.0).astype(BF16),
            jnp.where(low, 1.0, 0.0).astype(BF16),
            (((1,), (1,)), ((), ())),
            preferred_element_type=F32,
        )
        cnt[...] = count if i == 0 else cnt[...] + count
        fetch(i).wait()
        x = x_ref[i * width : (i + 1) * width, :]
        for p, s in enumerate(slots):
            part = dot(one_hot(packed, rows, (dom ^ s) * rows), x)
            acc[p] = part if i == 0 else acc[p] + part
    per = rows // LANES
    half = len(slots) // 2
    for p, s in enumerate(slots):
        tail[...] = jnp.zeros_like(tail)
        for h in range(per):
            c = cnt[pl.ds((dom ^ s) * per + h, 1), :]
            over = [c] + [jnp.floor((c + 0.5) * (1.0 / base**d)) for d in range(1, digits)]
            for d in range(digits):
                digit = over[d] if d == digits - 1 else over[d] - base * over[d + 1]
                tail[d * per + h : d * per + h + 1, 0:LANES] = digit
        out = keep_ref if p < half else send_ref
        at = (p % half) * (rows + EXTRA)
        out[at : at + rows, :] = acc[p].astype(out.dtype)
        out[at + rows : at + rows + EXTRA, :] = tail[...].astype(out.dtype)


def segment_sums(features, assign, slots, rows, base, digits):
    verts, feat = features.shape
    width = min(verts, 2048)
    half = len(slots) // 2
    shape = (half * (rows + EXTRA), feat)
    nodes = len(slots) * rows
    return pl.pallas_call(
        functools.partial(sums_kernel, slots=slots, rows=rows, base=base, digits=digits, width=width),
        out_shape=(
            jax.ShapeDtypeStruct(shape, F32),
            jax.ShapeDtypeStruct(shape, BF16),
            jax.ShapeDtypeStruct((verts, feat), BF16),
        ),
        in_specs=[ANY, ANY],
        out_specs=(VMEM, VMEM, VMEM),
        scratch_shapes=[
            pltpu.VMEM((1, verts), I32),
            pltpu.VMEM((len(slots), rows, feat), F32),
            pltpu.VMEM((max(16, nodes // LANES), LANES), F32),
            pltpu.VMEM((EXTRA, feat), F32),
            pltpu.SemaphoreType.DMA((verts // width + 1,)),
        ],
        compiler_params=pltpu.CompilerParams(vmem_limit_bytes=16 << 20),
        cost_estimate=cost(2 * nodes * verts * feat, verts * feat * 2),
        name="sums",
    )(in_hbm(assign.reshape(1, verts)), in_hbm(features))


def coarse_kernel(keep_ref, recv_ref, w_ref, out_ref, tail, *, rows, base, digits):
    per = rows // LANES
    feat = keep_ref.shape[1]
    tail[...] = keep_ref[rows:, :] + recv_ref[rows:, :].astype(F32)
    done = []
    for h in range(per):
        c = tail[h : h + 1, 0:LANES]
        for d in range(1, digits):
            c = c + tail[d * per + h : d * per + h + 1, 0:LANES] * float(base**d)
        root = jnp.sqrt(jnp.broadcast_to(c, (LANES, LANES)).T)
        at = slice(h * LANES, (h + 1) * LANES)
        total = keep_ref[at, :] + recv_ref[at, :].astype(F32)
        done.append(
            jnp.concatenate(
                [total[:, j : j + LANES] / root for j in range(0, feat, LANES)], axis=1
            ).astype(BF16)
        )
    out_ref[...] = dot(jnp.concatenate(done, axis=0), w_ref[...]).astype(BF16)


def coarse_part(keep, recv, w, rows, base, digits):
    feat = keep.shape[1]
    return pl.pallas_call(
        functools.partial(coarse_kernel, rows=rows, base=base, digits=digits),
        out_shape=jax.ShapeDtypeStruct((rows, feat), BF16),
        in_specs=[VMEM, VMEM, VMEM],
        out_specs=VMEM,
        scratch_shapes=[pltpu.VMEM((EXTRA, feat), F32)],
        compiler_params=pltpu.CompilerParams(vmem_limit_bytes=8 << 20),
        cost_estimate=cost(2 * rows * feat * feat, rows * feat * 8),
        name="coarse",
    )(keep, recv, w)


def mix_kernel(*refs, slots, rows, own, order):
    pa_ref, pb_ref, *pieces, out_ref, proj, wide, own_rows = refs
    dom = lax.axis_index("dom")
    me = dom * lax.axis_size("grp") + lax.axis_index("grp")
    half = len(slots) // 2
    for p, s in enumerate(slots):
        src = pa_ref if p < half else pb_ref
        value = src[(p % half) * rows : (p % half + 1) * rows, :]
        at = pl.multiple_of((dom ^ s) * rows, rows)
        proj[pl.ds(at, rows), :] = value
        wide[pl.ds(at, rows), :] = value.astype(F32)
    for q, t in enumerate(order):
        at = pl.multiple_of((me ^ t) * own, own)
        own_rows[q * own : (q + 1) * own, :] = wide[pl.ds(at, own), :]
    adj = jnp.concatenate([piece[...].astype(F32) for piece in pieces], axis=0).astype(BF16)
    out_ref[...] = (own_rows[...] + dot(adj, proj[...])).astype(BF16)


def mixed_rows(pa, pb, pieces, slots, rows, own, order):
    nodes, feat = len(slots) * rows, pa.shape[1]
    got = len(order) * own
    return pl.pallas_call(
        functools.partial(mix_kernel, slots=slots, rows=rows, own=own, order=order),
        out_shape=jax.ShapeDtypeStruct((got, feat), BF16),
        in_specs=[VMEM] * (2 + len(pieces)),
        out_specs=VMEM,
        scratch_shapes=[
            pltpu.VMEM((nodes, feat), BF16),
            pltpu.VMEM((nodes, feat), F32),
            pltpu.VMEM((got, feat), F32),
        ],
        compiler_params=pltpu.CompilerParams(vmem_limit_bytes=12 << 20),
        cost_estimate=cost(2 * got * nodes * feat, got * nodes * 2),
        name="mix",
    )(pa, pb, *pieces)


def join_kernel(a_ref, b_ref, out_ref):
    rows = a_ref.shape[0]
    out_ref[0:rows, :] = a_ref[...]
    out_ref[rows:, :] = b_ref[...]


def join(a, b):
    shape = (a.shape[0] + b.shape[0], a.shape[1])
    return pl.pallas_call(
        join_kernel,
        out_shape=jax.ShapeDtypeStruct(shape, a.dtype),
        in_specs=[VMEM, VMEM],
        out_specs=VMEM,
        compiler_params=pltpu.CompilerParams(vmem_limit_bytes=4 << 20),
        cost_estimate=cost(shape[0] * shape[1], shape[0] * shape[1] * 4),
        name="join",
    )(a, b)


def proj_kernel(low_idx, up_idx, x_ref, w_ref, own_ref, low_ref, up_ref, *, width):
    chunks = x_ref.shape[0] // width
    block = low_ref.shape[1]
    w = w_ref[...]
    for i in range(chunks):
        done = dot(x_ref[i * width : (i + 1) * width, :], w).astype(BF16)
        own_ref[i * (width // block) : (i + 1) * (width // block)] = done.reshape(width // block, block, done.shape[1])
    for h in range(low_ref.shape[0]):
        low_ref[h] = own_ref[low_idx[h]]
        up_ref[h] = own_ref[up_idx[h]]


def projection(send_lower, send_upper, features, w, block):
    verts, feat = features.shape
    halo = send_lower.shape[0]
    sent = jax.ShapeDtypeStruct((halo, block, feat), BF16)
    return pl.pallas_call(
        functools.partial(proj_kernel, width=min(verts, 1024)),
        out_shape=(jax.ShapeDtypeStruct((verts // block, block, feat), BF16), sent, sent),
        in_specs=[SMEM, SMEM, VMEM, VMEM],
        out_specs=(VMEM, VMEM, VMEM),
        compiler_params=pltpu.CompilerParams(vmem_limit_bytes=14 << 20),
        cost_estimate=cost(2 * verts * feat * feat, 4 * verts * feat),
        name="proj",
    )(send_lower, send_upper, features, w)


GROUP = 4
TURNS = 3
LAG = 2


def fine_kernel(cols_ref, live_ref, own_ref, below_ref, above_ref, adj_hbm, out_ref, ext, tiles, sems):
    rows, block = own_ref.shape[0], own_ref.shape[1]
    halo = below_ref.shape[0]

    def groups(r):
        return lax.div(live_ref[r] + (GROUP - 1), GROUP)

    most = tiles.shape[1] // GROUP

    def fetch(r, count):
        at = pl.ds(0, count * GROUP)
        return pltpu.make_async_copy(adj_hbm.at[r, at], tiles.at[r, at], sems.at[r])

    @pl.loop(0, rows)
    def _(r):
        lax.switch(groups(r) - 1, [lambda n=n: fetch(r, n).start() for n in range(1, most + 1)])

    ext[0:rows] = own_ref[...]
    ext[rows : rows + halo] = below_ref[...]
    ext[rows + halo :] = above_ref[...]

    def body(*accs):
        def push(columns):
            for q in range(2):
                rhs = jnp.concatenate([ext[c] for c in columns[2 * q : 2 * q + 2]], axis=0)
                pltpu.matmul_push_rhs(rhs, staging_register=0, mxu_index=q)

        def columns_of(r, i):
            return [cols_ref[i * GROUP + j, r] for j in range(GROUP)]

        def finish(r, turn):
            at = pl.ds(pl.multiple_of(r * block, block), block)
            out_ref[at, :] = pltpu.matmul_pop(accs[turn]) + pltpu.matmul_pop(accs[TURNS + turn])

        def row(r, turn, before):
            live = live_ref[r]
            following = jnp.minimum(r + 1, rows - 1)

            def with_groups(count):
                def run():
                    fetch(r, count).wait()
                    for i in range(count):
                        coming = columns_of(following, 0) if i + 1 == count else columns_of(r, i + 1)
                        for q in range(2):
                            lhs = []
                            for j in range(2):
                                k = i * GROUP + 2 * q + j
                                tile = tiles[r, k]
                                if i + 1 == count and 2 * q + j > 0:
                                    tile = jnp.where(k < live, tile, jnp.zeros_like(tile))
                                lhs.append(tile)
                            lhs = jnp.concatenate(lhs, axis=1)
                            pltpu.matmul_acc_lhs(accs[q * TURNS + turn], lhs, load_staged_rhs=0)
                        push(coming)
                        if i == 0 and before is not None:
                            finish(before, (turn + TURNS - LAG) % TURNS)

                return run

            lax.switch(groups(r) - 1, [with_groups(n) for n in range(1, most + 1)])

        push(columns_of(0, 0))
        for r in range(LAG):
            row(r, r % TURNS, None)

        @pl.loop(0, (rows - LAG) // TURNS)
        def _(h):
            for turn in range(TURNS):
                r = h * TURNS + turn + LAG
                row(r, (turn + LAG) % TURNS, r - LAG)

        for r in range((rows - LAG) // TURNS * TURNS + LAG, rows):
            row(r, r % TURNS, r - LAG)
        spare = rows % TURNS
        for q in range(2):
            zero = jnp.zeros((block, 2 * block), BF16)
            pltpu.matmul_acc_lhs(accs[q * TURNS + spare], zero, load_staged_rhs=0)
        for r in range(rows - LAG, rows):
            finish(r, r % TURNS)
        for q in range(2):
            ext[0, 0:16, :] = pltpu.matmul_pop(accs[q * TURNS + spare])[0:16].astype(BF16)

    shape = (block, 2 * block)
    pl.run_scoped(body, *[pltpu.ACC(q)(shape, F32) for q in range(2) for _ in range(TURNS)])


def fine_rows(tile_cols, tile_count, own, below, above, adj_tiles):
    rows, slots, block, _ = adj_tiles.shape
    feat = own.shape[2]
    halo = below.shape[0]
    assert slots % GROUP == 0 and rows % 2 == 0 and feat == 2 * block
    return pl.pallas_call(
        fine_kernel,
        out_shape=jax.ShapeDtypeStruct((rows * block, feat), F32),
        in_specs=[SMEM, SMEM, VMEM, VMEM, VMEM, ANY],
        out_specs=VMEM,
        scratch_shapes=[
            pltpu.VMEM((rows + 2 * halo, block, feat), BF16),
            pltpu.VMEM((rows, slots, block, block), BF16),
            pltpu.SemaphoreType.DMA((rows,)),
        ],
        compiler_params=pltpu.CompilerParams(vmem_limit_bytes=36 << 20),
        cost_estimate=cost(2 * rows * slots * block * block * feat, rows * slots * block * block * 2),
        name="fine",
    )(tile_cols.T, tile_count, own, below, above, in_hbm(adj_tiles))


def picked_rows(columns, m_ref, first):
    nodes = m_ref.shape[0]
    lane = (lax.broadcasted_iota(I32, (LANES, nodes), 1) + first).astype(I16)
    hots = []
    for column in columns:
        hot = jnp.concatenate([column] * (nodes // LANES), axis=1) == lane
        hots.append(jnp.where(hot, jnp.ones((), BF16), jnp.zeros((), BF16)))
    return dot(jnp.concatenate(hots, axis=0), m_ref[...])


def place_kernel(assign_ref, m_ref, fine_ref, out_ref, place_ref, *, own, gather_bits, width):
    me = lax.axis_index("dom") * lax.axis_size("grp") + lax.axis_index("grp")
    shift = own.bit_length() - 1
    assign = assign_ref[...]
    apart = lax.shift_right_logical(assign, shift) ^ me
    place = assign & (own - 1)
    for j, bit in enumerate(gather_bits):
        place = place + jnp.where((apart & bit) != 0, own << j, 0)
    place = place.astype(F32)
    for i in range(0, out_ref.shape[0], width):
        columns = []
        for j in range(i // LANES, (i + width) // LANES):
            column = jnp.broadcast_to(place[j : j + 1, :], (LANES, LANES)).T.astype(I32).astype(I16)
            place_ref[j * LANES : (j + 1) * LANES, :] = column
            columns.append(column)
        out_ref[i : i + width, :] = fine_ref[i : i + width, :] + picked_rows(columns, m_ref, 0)


def stored_columns(place_ref, start, width):
    return [place_ref[j : j + LANES, :] for j in range(start, start + width, LANES)]


def gain_kernel(place_ref, m_ref, fine_ref, out_ref, *, first, width):
    for i in range(0, out_ref.shape[0], width):
        columns = stored_columns(place_ref, i, width)
        out_ref[i : i + width, :] = fine_ref[i : i + width, :] + picked_rows(columns, m_ref, first)


def out_kernel(place_ref, m_ref, fine_ref, out_hbm, out_ref, sems, *, first, width):
    chunks = out_ref.shape[0] // width

    def store(i):
        at = pl.ds(i * width, width)
        return pltpu.make_async_copy(out_ref.at[at, :], out_hbm.at[at, :], sems.at[i])

    for i in range(chunks):
        at = slice(i * width, (i + 1) * width)
        picked = picked_rows(stored_columns(place_ref, i * width, width), m_ref, first)
        out_ref[at, :] = jnp.maximum(fine_ref[at, :] + picked, 0.0).astype(BF16)
        store(i).start()
    for i in range(chunks):
        store(i).wait()


def output_rows(assign, part_of, count, fine, own, gather_bits):
    verts, feat = fine.shape
    width = min(verts, 1024)
    place, first = None, 0
    for step in range(count):
        m = part_of(step)
        nodes = m.shape[0]
        shared = dict(
            compiler_params=pltpu.CompilerParams(vmem_limit_bytes=16 << 20),
            cost_estimate=cost(2 * verts * nodes * feat, verts * feat * 6),
        )
        wide = jax.ShapeDtypeStruct((verts, feat), F32)
        if step == 0:
            fine, place = pl.pallas_call(
                functools.partial(place_kernel, own=own, gather_bits=gather_bits, width=width),
                out_shape=(wide, jax.ShapeDtypeStruct((verts, LANES), I16)),
                in_specs=[VMEM] * 3,
                out_specs=(VMEM, VMEM),
                name="place",
                **shared,
            )(assign.reshape(verts // LANES, LANES), m, fine)
        elif step + 1 < count:
            fine = pl.pallas_call(
                functools.partial(gain_kernel, first=first, width=width),
                out_shape=wide,
                in_specs=[VMEM] * 3,
                out_specs=VMEM,
                name="gain",
                **shared,
            )(place, m, fine)
        else:
            return pl.pallas_call(
                functools.partial(out_kernel, first=first, width=width),
                out_shape=jax.ShapeDtypeStruct((verts, feat), BF16),
                in_specs=[VMEM] * 3,
                out_specs=ANY,
                scratch_shapes=[pltpu.VMEM((verts, feat), BF16), pltpu.SemaphoreType.DMA((verts // width,))],
                name="out",
                **shared,
            )(place, m, fine)
        first += nodes


def spread(x, dom_bits, grps, flip):
    parts = [x]
    bits = dom_bits[:0:-1] + dom_bits[:1]
    for step, bit in enumerate(bits):
        parts.append(flip(x, bit * grps))
        if step + 1 < len(bits):
            x = join(x, parts[-1])
    return x, parts


def layer(
    features,
    w_fine,
    adj_tiles,
    tile_cols,
    tile_count,
    send_lower,
    send_upper,
    assign,
    w_coarse,
    coarse_adj,
):
    verts, _ = features.shape
    block = adj_tiles.shape[2]
    own, nodes = coarse_adj.shape
    doms, grps = lax.axis_size("dom"), lax.axis_size("grp")
    devices = doms * grps
    dom_bits, grp_bits = bits_of(doms), bits_of(grps)
    rows = nodes // doms

    def flip(x, bit):
        return lax.ppermute(x, AXES, [(i, i ^ bit) for i in range(devices)])

    base = 256 // devices + 1
    digits = 1
    while base**digits <= verts:
        digits += 1

    slots = [0]
    for bit in dom_bits[::-1]:
        slots = slots + [s ^ bit for s in slots]

    gather_bits = grp_bits[:1:-1] + grp_bits[:1] + grp_bits[1:2]
    order = [0]
    for bit in gather_bits:
        order = order + [t ^ bit for t in order]
    pieces, coming = [coarse_adj], coarse_adj
    for step, bit in enumerate(gather_bits):
        pieces.append(flip(coming, bit))
        if step + 1 < len(gather_bits):
            coming = join(coming, pieces[-1])

    keep, send, held = segment_sums(features, assign, slots, rows, base, digits)
    for step, bit in enumerate(dom_bits):
        recv = flip(send, bit * grps)
        if step + 1 < len(dom_bits):
            total = keep + recv.astype(F32)
            half = total.shape[0] // 2
            keep, send = total[:half], total[half:].astype(BF16)

    projected, low, up = projection(send_lower, send_upper, held, w_fine, block)
    going_up = [(i, (i + 1) % doms) for i in range(doms)]
    from_below = lax.ppermute(up, "dom", going_up)
    from_above = lax.ppermute(low, "dom", [(j, i) for i, j in going_up])
    fine = fine_rows(tile_cols, tile_count, projected, from_below, from_above, adj_tiles)

    for bit in grp_bits:
        keep = keep + recv.astype(F32)
        recv = flip(keep.astype(BF16), bit)
    proj = coarse_part(keep, recv, w_coarse, rows, base, digits)
    proj, parts = spread(proj, dom_bits, grps, flip)
    mixed = mixed_rows(proj, parts[-1], pieces, slots, rows, own, order)
    _, parts = spread(mixed, dom_bits, grps, flip)
    all_bits = gather_bits + [b * grps for b in dom_bits[:0:-1] + dom_bits[:1]]
    return output_rows(assign, lambda i: parts[i], len(parts), fine, own, all_bits)


def solution(mesh):
    return jax.shard_map(
        layer,
        mesh=mesh,
        in_specs=(
            P(AXES, None),
            P(),
            P(AXES, None, None, None),
            P(AXES, None),
            P(AXES),
            P(AXES),
            P(AXES),
            P(AXES),
            P(),
            P(AXES, None),
        ),
        out_specs=P(AXES, None),
        check_vma=False,
    )
```
